32 devices in a mesh: tile: 16 (over z, y, core), cam: 2 (over x).
Axes of the slice: x: 2, y: 2, z: 4, core: 2. Of those that a mesh axis runs over, the one named last changes fastest.
Arguments:
- features: bfloat16 [6144, 256], P(('tile', 'cam')), may hold values from -6 to 6
- value_weight: bfloat16 [256, 256], replicated, may hold values from -0.375 to 0.375
- output_weight: bfloat16 [256, 256], replicated, may hold values from -0.375 to 0.375
- hit_list: int32 [16, 2], P('tile'), may hold values from 0 to 5, as said below
- sample_index: int32 [8192, 2, 64], P('tile'), may hold values from 0 to 1023, as said below
- attention: bfloat16 [8192, 64], P('tile'), may hold values from 0.0099487305 to 1
- validity: int32 [8192, 2], P('tile'), may hold values from 0 to 1, as said below
Outputs:
- projected: bfloat16 [8192, 256], P(('tile', 'cam'))
The draws below stay inside these ranges and needn't reach their ends.
Inputs may be any that keep to these rules, and one draw needn't show every extreme that they name: `hit_list`: camera numbers 0 to 5; where a tile sees one camera its two entries are equal. `validity`: where a tile's two hit_list entries are equal, the second column is 0 for every query of that tile. `sample_index`: for one query, slot and head, the 8 entries h * 8 to h * 8 + 7 all differ.
All inputs are finite; a program needn't handle non-finite values.
Results may differ from the reference program's by a relative error of at most 0.0058.
Values may be sent and summed in bfloat16 or wider, within the bound.
A program may use at most 64 MiB of HBM per device.

```python
import math
import jax
import jax.numpy as jnp
from jax import lax

D = 256
H = 8
K = 8
HITS = 2
CAMS = 6
CAM_ROWS = 1024
Q_TILE = 512
TILES = 16
QUERIES = 8192
FEATURE_ROWS = 6144


def camera_pairs(key):
    base_key = jax.random.fold_in(key, 7)
    lead_key, stride_key, lone_key = jax.random.split(base_key, 3)
    leading = jax.random.randint(lead_key, (TILES,), 0, CAMS)
    stride = jax.random.randint(stride_key, (TILES,), 1, CAMS)
    lonely = jax.random.randint(lone_key, (TILES,), 0, 3) == 0
    partner = jnp.where(lonely, leading, (leading + stride) % CAMS)
    return jnp.stack([leading, partner], axis=1).astype(jnp.int32)


def draw_hit_list(key, part):
    return camera_pairs(key)


def draw_validity(key, part):
    pairs = camera_pairs(key)
    query_cams = jnp.repeat(pairs, Q_TILE, axis=0)
    first_key, second_key = jax.random.split(jax.random.fold_in(key, 19))
    leading_live = jax.random.randint(first_key, (QUERIES,), 0, 5) != 0
    second_live = jax.random.randint(second_key, (QUERIES,), 0, 5) < 3
    second_live = second_live & (query_cams[:, 1] != query_cams[:, 0])
    return jnp.stack([leading_live, second_live], axis=1).astype(jnp.int32)


def draw_sample_index(key, part):
    center_key, jitter_key = jax.random.split(jax.random.fold_in(key, 31))
    spacing = CAM_ROWS // K
    center = jax.random.randint(center_key, (QUERIES, HITS, H, 1), 0, CAM_ROWS)
    jitter = jax.random.randint(jitter_key, (QUERIES, HITS, H, K), 0, spacing)
    strides = jnp.arange(K).reshape(1, 1, 1, K) * spacing
    return ((center + strides + jitter) % CAM_ROWS).reshape(QUERIES, HITS, H * K).astype(jnp.int32)


def shard_levels(key, extent, pieces, smallest, high):
    loudness = 1.0
    for dim, blocks in pieces:
        steps = jax.random.uniform(jax.random.fold_in(jax.random.fold_in(key, 6), dim), (blocks,), jnp.float32, smallest / len(pieces), high / len(pieces))
        loudness = loudness * jnp.repeat(jnp.exp(steps), extent[dim] // blocks).reshape((-1,) + (1,) * (len(extent) - 1 - dim))
    return loudness


def normal_values(rng, extent, width, limit, shards=(), kind=jnp.bfloat16):
    entries = width * jax.random.normal(rng, extent, jnp.float32)
    if shards:
        entries = entries * shard_levels(rng, extent, shards, -0.22, 0.18)
    return jnp.clip(entries, -limit, limit).astype(kind)


def setup_inputs(seed: int = 0) -> dict:
    arg_keys = jax.random.split(jax.random.key(seed), 8)
    return {
        "features": normal_values(arg_keys[0], (FEATURE_ROWS, D), 1.0, 6.0, ((0, 32),)),
        "value_weight": normal_values(arg_keys[1], (D, D), D ** -0.5, 0.375),
        "output_weight": normal_values(arg_keys[2], (D, D), D ** -0.5, 0.375),
        "hit_list": draw_hit_list(jax.random.fold_in(arg_keys[7], 71), 0),
        "sample_index": draw_sample_index(jax.random.fold_in(arg_keys[7], 71), 0),
        "attention": jnp.clip(jnp.exp(math.log(1.0) - 4.61031033 * jax.random.uniform(arg_keys[5], (QUERIES, H * K), jnp.float32) ** shard_levels(arg_keys[5], (QUERIES, H * K), ((0, 16),), -0.2, 0.2)), 0.0099487305, 1.0).astype(jnp.bfloat16),
        "validity": draw_validity(jax.random.fold_in(arg_keys[7], 71), 0),
    }


def reference(features, value_weight, output_weight, hit_list, sample_index, attention, validity):
    values = jnp.dot(features, value_weight, preferred_element_type=jnp.float32).astype(jnp.bfloat16)
    value_heads = values.astype(jnp.float32).reshape(-1, H, D // H)
    hit_count = jnp.sum(validity, axis=1)
    inverse = 1.0 / jnp.maximum(hit_count, 1).astype(jnp.float32)
    weights = attention.astype(jnp.float32).reshape(-1, 1, H, K) * validity.astype(jnp.float32)[:, :, None, None]
    weights = weights * inverse[:, None, None, None]
    cameras = jnp.repeat(hit_list, Q_TILE, axis=0).astype(jnp.int32)
    targets = (cameras[:, :, None] * CAM_ROWS + sample_index).astype(jnp.int32)
    targets = targets.reshape(TILES, Q_TILE, HITS, H, K)
    weights = weights.reshape(TILES, Q_TILE, HITS, H, K)
    head_ids = jnp.arange(H).astype(jnp.int32).reshape(1, 1, H, 1)

    def per_tile(tile_pair):
        tile_targets, tile_weights = tile_pair
        picked = value_heads[tile_targets, head_ids]
        return jnp.sum(tile_weights[..., None] * picked, axis=(1, 3))

    sampled = lax.map(per_tile, (targets, weights)).reshape(TILES * Q_TILE, D)
    attended = sampled.astype(jnp.bfloat16)
    return jnp.dot(attended, output_weight, preferred_element_type=jnp.float32).astype(jnp.bfloat16)
```

```python
import functools

import jax
import jax.numpy as jnp
from jax import lax
from jax.experimental import pallas as pl
from jax.experimental.pallas import tpu as pltpu
from jax.sharding import PartitionSpec as P

H = 8
K = 8
HITS = 2
CAM_ROWS = 1024
LANES = 128
MESH = pl.DeviceIdType.MESH


def gather_kernel(depth, v_ref, G, recv, sx, sup, sdn, sy, sc):
    me = lax.axis_index("tile")
    x = lax.axis_index("cam")
    core = lax.rem(me, 2)
    y = lax.rem(me // 2, 2)
    z = me // 4
    rows = v_ref.shape[1]

    def place(zz, yy, cc):
        return (zz * 2 + yy) * 2 + cc

    def block_of(zz, yy, cc, b):
        return place(zz, yy, cc) * 2 + b

    def span(blk):
        return pl.ds(pl.multiple_of(blk * rows, 16), rows)

    has_up = z < depth - 1
    has_down = z > 0
    x_peer = (me, 1 - x)
    y_peer = (place(z, 1 - y, core), x)
    c_peer = (place(z, y, 1 - core), x)
    up_peer = (place(jnp.minimum(z + 1, depth - 1), y, core), x)
    down_peer = (place(jnp.maximum(z - 1, 0), y, core), x)

    barrier = pltpu.get_barrier_semaphore()
    for peer in (x_peer, y_peer, c_peer):
        pl.semaphore_signal(barrier, inc=1, device_id=peer, device_id_type=MESH)

    @pl.when(has_up)
    def _():
        pl.semaphore_signal(barrier, inc=1, device_id=up_peer, device_id_type=MESH)

    @pl.when(has_down)
    def _():
        pl.semaphore_signal(barrier, inc=1, device_id=down_peer, device_id_type=MESH)

    pl.semaphore_wait(barrier, 3 + has_up.astype(jnp.int32) + has_down.astype(jnp.int32))

    def copy(src, blk, send, peer):
        return pltpu.make_async_remote_copy(
            src_ref=src,
            dst_ref=G.at[span(blk)],
            send_sem=send,
            recv_sem=recv.at[blk],
            device_id=peer,
            device_id_type=MESH,
        )

    def arrived(blk):
        copy(G.at[span(blk)], blk, sx.at[0], x_peer).wait_recv()

    own = block_of(z, y, core, x)
    copy(v_ref.at[1 - x], own, sx.at[0], x_peer).start()

    def send_up(src, blk, slot):
        copy(src, blk, sup.at[slot], up_peer).start()

    def send_down(src, blk, slot):
        copy(src, blk, sdn.at[slot], down_peer).start()

    def line_step(distance):
        for sign in (1, -1) if distance else (0,):
            zz = z - sign * distance
            live = (zz >= 0) & (zz < depth)
            for b in (0, 1):
                half = x if b == 0 else 1 - x

                def go(zz=zz, half=half, b=b, sign=sign):
                    blk = block_of(zz, y, core, half)
                    if distance == 0 and b == 0:
                        src = v_ref.at[x]
                    else:
                        arrived(blk)
                        src = G.at[span(blk)]
                    slot = zz * 2 + half
                    copy(src, blk, sy.at[slot], y_peer).start()
                    if sign >= 0:
                        pl.when(has_up)(lambda: send_up(src, blk, slot))
                    if sign <= 0:
                        pl.when(has_down)(lambda: send_down(src, blk, slot))
                    copy(src, blk, sc.at[slot], c_peer).start()

                if distance:
                    pl.when(live)(go)
                else:
                    go()

    def across_step(distance):
        for sign in (1, -1) if distance else (0,):
            zz = z - sign * distance
            live = (zz >= 0) & (zz < depth)
            for b in (0, 1):
                half = x if b == 0 else 1 - x

                def go(zz=zz, half=half):
                    blk = block_of(zz, 1 - y, core, half)
                    arrived(blk)
                    slot = depth * 2 + zz * 2 + half
                    copy(G.at[span(blk)], blk, sc.at[slot], c_peer).start()

                if distance:
                    pl.when(live)(go)
                else:
                    go()

    for distance in range(depth):
        line_step(distance)
        if distance:
            across_step(distance - 1)
    G[span(own), :] = v_ref[x]
    across_step(depth - 1)

    for zz in range(depth):
        for yy in (0, 1):
            for b in (0, 1):
                arrived(block_of(zz, yy, 1 - core, b))

    def sent(sem):
        copy(v_ref.at[0], own, sem, x_peer).wait_send()

    sent(sx.at[0])
    for slot in range(depth * 2):
        zz = slot // 2
        sent(sy.at[slot])
        pl.when(has_up & (zz <= z))(lambda slot=slot: sent(sup.at[slot]))
        pl.when(has_down & (zz >= z))(lambda slot=slot: sent(sdn.at[slot]))
    for slot in range(depth * 4):
        sent(sc.at[slot])


def gather_values(halves, tiles):
    depth = tiles // 4
    _, rows, width = halves.shape
    blocks = tiles * 2
    dma = pltpu.SemaphoreType.DMA
    return pl.pallas_call(
        functools.partial(gather_kernel, depth),
        out_shape=jax.ShapeDtypeStruct((blocks * rows, width), jnp.bfloat16),
        in_specs=[pl.BlockSpec(memory_space=pltpu.VMEM)],
        out_specs=pl.BlockSpec(memory_space=pltpu.VMEM),
        scratch_shapes=[
            dma((blocks,)),
            dma((1,)),
            dma((depth * 2,)),
            dma((depth * 2,)),
            dma((depth * 2,)),
            dma((depth * 4,)),
        ],
        compiler_params=pltpu.CompilerParams(collective_id=0, has_side_effects=True),
    )(halves)


def lane_pick(source, index):
    return jnp.take_along_axis(source, index, axis=1, mode="promise_in_bounds")


def sample_kernel(heads, hit_ref, vals_ref, idx_ref, attn_ref, factor_ref, out_ref, table, summed):
    width = vals_ref.shape[1]
    head_width = width // heads
    queries = idx_ref.shape[1]
    groups = queries // LANES
    parts = CAM_ROWS // LANES
    for s in range(HITS):
        for j in range(parts):
            first = pl.multiple_of(hit_ref[0, s] * CAM_ROWS + j * LANES, LANES)
            block = vals_ref[pl.ds(first, LANES), :].astype(jnp.float32)
            table[s * parts + j] = block.T

    def one(step, _):
        g = step // heads
        h = lax.rem(step, heads)
        lanes = pl.ds(pl.multiple_of(g * LANES, LANES), LANES)
        cols = pl.ds(pl.multiple_of(h * head_width, head_width), head_width)
        attn = attn_ref[pl.ds(pl.multiple_of(h * K, K), K), lanes]
        acc = jnp.zeros((head_width, LANES), jnp.float32)
        for s in range(HITS):
            index = idx_ref[pl.ds(pl.multiple_of(s * heads * K + h * K, K), K), lanes]
            low = index % LANES
            high = index // LANES
            weight = attn * factor_ref[s : s + 1, lanes]
            for k in range(K):
                lo = jnp.broadcast_to(low[k : k + 1], (head_width, LANES))
                hi = jnp.broadcast_to(high[k : k + 1], (head_width, LANES))
                picked = jnp.zeros((head_width, LANES), jnp.float32)
                for j in range(parts):
                    got = lane_pick(table[s * parts + j, cols, :], lo)
                    picked = jnp.where(hi == j, got, picked)
                acc = acc + weight[k : k + 1] * picked
        summed[cols, :] = acc

        @pl.when(h == heads - 1)
        def _():
            rows = pl.ds(pl.multiple_of(g * LANES, LANES), LANES)
            out_ref[rows, :] = summed[...].T.astype(out_ref.dtype)

        return 0

    lax.fori_loop(0, groups * heads, one, 0)


def sample(hit_list, vals, index, attention, validity, heads):
    queries = index.shape[0]
    width = vals.shape[1]
    padded = -(-queries // LANES) * LANES
    index = index.reshape(queries, HITS * heads * K).T
    attention = attention.astype(jnp.float32).T
    count = jnp.maximum(jnp.sum(validity, axis=1, keepdims=True), 1)
    factor = (validity.astype(jnp.float32) / count.astype(jnp.float32)).T
    pad = ((0, 0), (0, padded - queries))
    index, attention, factor = (jnp.pad(a, pad) for a in (index, attention, factor))
    out = pl.pallas_call(
        functools.partial(sample_kernel, heads),
        out_shape=jax.ShapeDtypeStruct((padded, width), jnp.bfloat16),
        in_specs=[pl.BlockSpec(memory_space=pltpu.SMEM)]
        + [pl.BlockSpec(memory_space=pltpu.VMEM)] * 4,
        out_specs=pl.BlockSpec(memory_space=pltpu.VMEM),
        scratch_shapes=[
            pltpu.VMEM((HITS * CAM_ROWS // LANES, width, LANES), jnp.float32),
            pltpu.VMEM((width, LANES), jnp.float32),
        ],
    )(hit_list, vals, index, attention, factor)
    return out[:queries]


def project_kernel(a_ref, w_ref, out_ref, other, send, recv):
    me = lax.axis_index("tile")
    x = lax.axis_index("cam")
    rows = out_ref.shape[0]
    width = a_ref.shape[1]
    peer = (me, 1 - x)
    barrier = pltpu.get_barrier_semaphore()
    pl.semaphore_signal(barrier, inc=1, device_id=peer, device_id_type=MESH)
    pl.semaphore_wait(barrier, 1)
    copy = pltpu.make_async_remote_copy(
        src_ref=a_ref.at[pl.ds(pl.multiple_of((1 - x) * rows, rows), rows)],
        dst_ref=other,
        send_sem=send,
        recv_sem=recv,
        device_id=peer,
        device_id_type=MESH,
    )
    copy.start()
    mine = a_ref[pl.ds(pl.multiple_of(x * rows, rows), rows), :]
    near = w_ref[pl.ds(pl.multiple_of(x * width, width), width), :]
    far = w_ref[pl.ds(pl.multiple_of((1 - x) * width, width), width), :]
    total = jnp.dot(mine, near, preferred_element_type=jnp.float32)
    copy.wait()
    total = total + jnp.dot(other[...], far, preferred_element_type=jnp.float32)
    out_ref[...] = total.astype(out_ref.dtype)


def project(attended, output_weight):
    rows = attended.shape[0] // 2
    return pl.pallas_call(
        project_kernel,
        out_shape=jax.ShapeDtypeStruct((rows, output_weight.shape[1]), jnp.bfloat16),
        in_specs=[pl.BlockSpec(memory_space=pltpu.VMEM)] * 2,
        out_specs=pl.BlockSpec(memory_space=pltpu.VMEM),
        scratch_shapes=[
            pltpu.VMEM((rows, attended.shape[1]), jnp.bfloat16),
            pltpu.SemaphoreType.DMA,
            pltpu.SemaphoreType.DMA,
        ],
        compiler_params=pltpu.CompilerParams(collective_id=1, has_side_effects=True),
    )(attended, output_weight)


def body(features, value_weight, output_weight, hit_list, sample_index, attention, validity):
    values = jnp.dot(features, value_weight, preferred_element_type=jnp.float32).astype(
        jnp.bfloat16
    )
    tiles = lax.axis_size("tile")
    cams = lax.axis_size("cam")
    place = lax.axis_index("cam")
    queries = sample_index.shape[0]
    width = values.shape[1]
    if cams == 2 and tiles % 4 == 0 and width == 2 * LANES and features.shape[0] % 16 == 0:
        heads = H // 2
        halves = jnp.stack([values[:, :LANES], values[:, LANES:]])
        vals = gather_values(halves, tiles)
        index = lax.dynamic_slice_in_dim(sample_index, place * heads * K, heads * K, 2)
        weights = lax.dynamic_slice_in_dim(attention, place * heads * K, heads * K, 1)
        attended = sample(hit_list, vals, index, weights, validity, heads)
        return project(attended, output_weight)
    else:
        share = queries // cams
        everything = lax.all_gather(values, ("tile", "cam"), axis=0, tiled=True)
        index, weights, valid = (
            lax.dynamic_slice_in_dim(a, place * share, share, 0)
            for a in (sample_index, attention, validity)
        )
        attended = sample(hit_list, everything, index, weights, valid, H)
    return jnp.dot(attended, output_weight, preferred_element_type=jnp.float32).astype(jnp.bfloat16)


def solution(mesh):
    in_specs = (
        P(("tile", "cam"), None),
        P(),
        P(),
        P("tile", None),
        P("tile", None, None),
        P("tile", None),
        P("tile", None),
    )
    out_specs = P(("tile", "cam"), None)
    return jax.shard_map(body, mesh=mesh, in_specs=in_specs, out_specs=out_specs, check_vma=False)
```

```python
import functools

import jax
import jax.numpy as jnp
from jax import lax
from jax.experimental import pallas as pl
from jax.experimental.pallas import tpu as pltpu
from jax.sharding import PartitionSpec as P

H = 8
K = 8
HITS = 2
CAM_ROWS = 1024
LANES = 128
MESH = pl.DeviceIdType.MESH


def gather_kernel(depth, v_ref, G, recv, sx, sz, sy, sc):
    me = lax.axis_index("tile")
    x = lax.axis_index("cam")
    core = lax.rem(me, 2)
    y = lax.rem(me // 2, 2)
    z = me // 4
    rows, width = G.shape[0] // (depth * 8), G.shape[1]

    def half_of(index):
        return v_ref.at[:, pl.ds(pl.multiple_of(index * width, width), width)]

    def place(zz, yy, cc):
        return (zz * 2 + yy) * 2 + cc

    def block_of(zz, yy, cc, b):
        return place(zz, yy, cc) * 2 + b

    def span(blk):
        return pl.ds(pl.multiple_of(blk * rows, 16), rows)

    has_up = z < depth - 1
    has_down = z > 0
    x_peer = (me, 1 - x)
    y_peer = (place(z, 1 - y, core), x)
    c_peer = (place(z, y, 1 - core), x)
    has_up2 = z < depth - 2
    has_down2 = z > 1
    up_peer = (place(jnp.minimum(z + 1, depth - 1), y, core), x)
    down_peer = (place(jnp.maximum(z - 1, 0), y, core), x)
    up2_peer = (place(jnp.minimum(z + 2, depth - 1), y, core), x)
    down2_peer = (place(jnp.maximum(z - 2, 0), y, core), x)
    line = (
        (has_up2, up2_peer),
        (has_down2, down2_peer),
        (has_up, up_peer),
        (has_down, down_peer),
    )

    barrier = pltpu.get_barrier_semaphore()
    for peer in (x_peer, y_peer, c_peer):
        pl.semaphore_signal(barrier, inc=1, device_id=peer, device_id_type=MESH)

    peers = 3
    for exists, peer in line:
        peers = peers + exists.astype(jnp.int32)

        @pl.when(exists)
        def _(peer=peer):
            pl.semaphore_signal(barrier, inc=1, device_id=peer, device_id_type=MESH)

    pl.semaphore_wait(barrier, peers)

    def copy(src, blk, send, peer):
        return pltpu.make_async_remote_copy(
            src_ref=src,
            dst_ref=G.at[span(blk)],
            send_sem=send,
            recv_sem=recv.at[blk],
            device_id=peer,
            device_id_type=MESH,
        )

    def arrived(blk):
        copy(G.at[span(blk)], blk, sx.at[0], x_peer).wait_recv()

    own = block_of(z, y, core, x)
    copy(half_of(1 - x), own, sx.at[0], x_peer).start()

    def send_line(which, src, blk, slot):
        exists, peer = line[which]

        @pl.when(exists)
        def _():
            copy(src, blk, sz.at[slot], peer).start()

    def line_step(distance):
        for sign in (1, -1) if distance else (0,):
            zz = z - sign * distance
            live = (zz >= 0) & (zz < depth)
            for b in (0, 1):
                half = x if b == 0 else 1 - x

                def go(zz=zz, half=half, b=b, sign=sign):
                    blk = block_of(zz, y, core, half)
                    if distance == 0 and b == 0:
                        src = half_of(x)
                    else:
                        arrived(blk)
                        src = G.at[span(blk)]
                    slot = zz * 2 + half
                    if distance == 0:
                        for which in range(4):
                            send_line(which, src, blk, which * 2 + b)
                    elif distance == 2:
                        which = 2 if sign > 0 else 3
                        send_line(which, src, blk, 4 + which * 2 + b)
                    copy(src, blk, sy.at[slot], y_peer).start()
                    copy(src, blk, sc.at[slot], c_peer).start()

                if distance:
                    pl.when(live)(go)
                else:
                    go()

    def across_step(distance):
        for sign in (1, -1) if distance else (0,):
            zz = z - sign * distance
            live = (zz >= 0) & (zz < depth)
            for b in (0, 1):
                half = x if b == 0 else 1 - x

                def go(zz=zz, half=half):
                    blk = block_of(zz, 1 - y, core, half)
                    arrived(blk)
                    slot = depth * 2 + zz * 2 + half
                    copy(G.at[span(blk)], blk, sc.at[slot], c_peer).start()

                if distance:
                    pl.when(live)(go)
                else:
                    go()

    for distance in range(depth):
        line_step(distance)
        if distance:
            across_step(distance - 1)
    G[span(own), :] = v_ref[:, pl.ds(pl.multiple_of(x * width, width), width)]
    across_step(depth - 1)

    for zz in range(depth):
        for yy in (0, 1):
            for b in (0, 1):
                arrived(block_of(zz, yy, 1 - core, b))

    def sent(sem):
        copy(half_of(0), own, sem, x_peer).wait_send()

    sent(sx.at[0])
    for slot in range(depth * 2):
        sent(sy.at[slot])
    for b in (0, 1):
        for which in range(4):
            pl.when(line[which][0])(lambda i=which * 2 + b: sent(sz.at[i]))
        pl.when(has_up & has_down2)(lambda b=b: sent(sz.at[8 + b]))
        pl.when(has_down & has_up2)(lambda b=b: sent(sz.at[10 + b]))
    for slot in range(depth * 4):
        sent(sc.at[slot])


def gather_values(values, tiles):
    depth = tiles // 4
    rows, width = values.shape[0], values.shape[1] // 2
    blocks = tiles * 2
    dma = pltpu.SemaphoreType.DMA
    return pl.pallas_call(
        functools.partial(gather_kernel, depth),
        out_shape=jax.ShapeDtypeStruct((blocks * rows, width), jnp.bfloat16),
        in_specs=[pl.BlockSpec(memory_space=pltpu.VMEM)],
        out_specs=pl.BlockSpec(memory_space=pltpu.VMEM),
        scratch_shapes=[
            dma((blocks,)),
            dma((1,)),
            dma((12,)),
            dma((depth * 2,)),
            dma((depth * 4,)),
        ],
        compiler_params=pltpu.CompilerParams(collective_id=0, has_side_effects=True),
    )(values)


def lane_pick(source, index):
    return jnp.take_along_axis(source, index, axis=1, mode="promise_in_bounds")


def sample_kernel(
    heads, pair, hit_ref, head_ref, vals_ref, idx_ref, attn_ref, valid_ref, out_ref, table, attns, summed
):
    width = vals_ref.shape[1]
    head_width = width // heads
    queries = idx_ref.shape[1]
    groups = queries // LANES
    parts = CAM_ROWS // LANES
    for s in range(HITS):
        for j in range(parts):
            first = pl.multiple_of(hit_ref[0, s] * CAM_ROWS + j * LANES, LANES)
            block = vals_ref[pl.ds(first, LANES), :].astype(jnp.float32)
            table[s * parts + j] = block.T
    attns[...] = attn_ref[...].astype(jnp.float32)

    def one(step, _):
        g = step * pair // heads
        lanes = pl.ds(pl.multiple_of(g * LANES, LANES), LANES)
        valid = valid_ref[:, lanes]
        count = jnp.maximum(jnp.sum(valid, axis=0, keepdims=True), 1)
        factor = valid.astype(jnp.float32) * (1.0 / count.astype(jnp.float32))
        for e in range(pair):
            h = lax.rem(step * pair, heads) + e
            attn = attns[pl.ds(pl.multiple_of((head_ref[0] + h) * K, K), K), lanes]
            acc = [jnp.zeros((8, LANES), jnp.float32)] * (head_width // 8)
            for s in range(HITS):
                index = idx_ref[pl.ds(pl.multiple_of(s * heads * K + h * K, K), K), lanes]
                low = index & (LANES - 1)
                high = index // LANES
                weight = attn * factor[s : s + 1]
                for k in range(K):
                    lo = jnp.broadcast_to(low[k : k + 1], (8, LANES))
                    hi = jnp.broadcast_to(high[k : k + 1], (8, LANES))
                    wt = jnp.broadcast_to(weight[k : k + 1], (8, LANES))
                    masks = [hi == j for j in range(parts)]
                    for d in range(head_width // 8):
                        cols = pl.ds(pl.multiple_of(h * head_width + d * 8, 8), 8)
                        picked = lane_pick(table[s * parts, cols, :], lo)
                        for j in range(1, parts):
                            got = lane_pick(table[s * parts + j, cols, :], lo)
                            picked = jnp.where(masks[j], got, picked)
                        acc[d] = acc[d] + wt * picked
            for d in range(head_width // 8):
                summed[pl.ds(pl.multiple_of(h * head_width + d * 8, 8), 8), :] = acc[d]

        @pl.when(lax.rem(step * pair, heads) == heads - pair)
        def _():
            rows = pl.ds(pl.multiple_of(g * LANES, LANES), LANES)
            out_ref[rows, :] = summed[...].T.astype(out_ref.dtype)

        return 0

    lax.fori_loop(0, groups * heads // pair, one, 0)


def sample(hit_list, vals, index, attention, validity, heads, first_head):
    queries = index.shape[0]
    width = vals.shape[1]
    padded = -(-queries // LANES) * LANES
    index = index.reshape(queries, HITS * heads * K).T
    extra = padded - queries
    index = jnp.pad(index, ((0, 0), (0, extra)))
    validity = jnp.pad(validity.T, ((0, 0), (0, extra)))
    attention = jnp.pad(attention.T, ((0, 0), (0, extra)))
    pair = 2 if heads % 2 == 0 else 1
    first_head = jnp.reshape(first_head, (1,)).astype(jnp.int32)
    out = pl.pallas_call(
        functools.partial(sample_kernel, heads, pair),
        out_shape=jax.ShapeDtypeStruct((padded, width), jnp.bfloat16),
        in_specs=[pl.BlockSpec(memory_space=pltpu.SMEM)] * 2
        + [pl.BlockSpec(memory_space=pltpu.VMEM)] * 4,
        out_specs=pl.BlockSpec(memory_space=pltpu.VMEM),
        scratch_shapes=[
            pltpu.VMEM((HITS * CAM_ROWS // LANES, width, LANES), jnp.float32),
            pltpu.VMEM(attention.shape, jnp.float32),
            pltpu.VMEM((width, LANES), jnp.float32),
        ],
    )(hit_list, first_head, vals, index, attention, validity)
    return out[:queries]


def exchange_kernel(a_ref, out_ref, local, send, recv):
    me = lax.axis_index("tile")
    x = lax.axis_index("cam")
    rows = out_ref.shape[0]
    width = a_ref.shape[1]
    peer = (me, 1 - x)
    barrier = pltpu.get_barrier_semaphore()
    pl.semaphore_signal(barrier, inc=1, device_id=peer, device_id_type=MESH)
    pl.semaphore_wait(barrier, 1)

    def share(index):
        return a_ref.at[pl.ds(pl.multiple_of(index * rows, rows), rows)]

    mine = out_ref.at[:, pl.ds(pl.multiple_of(x * width, width), width)]
    copy = pltpu.make_async_remote_copy(
        src_ref=share(1 - x),
        dst_ref=mine,
        send_sem=send,
        recv_sem=recv,
        device_id=peer,
        device_id_type=MESH,
    )
    copy.start()
    keep = pltpu.make_async_copy(share(x), mine, local)
    keep.start()
    keep.wait()
    copy.wait()


def exchange(attended):
    queries, width = attended.shape
    dma = pltpu.SemaphoreType.DMA
    return pl.pallas_call(
        exchange_kernel,
        out_shape=jax.ShapeDtypeStruct((queries // 2, width * 2), jnp.bfloat16),
        in_specs=[pl.BlockSpec(memory_space=pltpu.VMEM)],
        out_specs=pl.BlockSpec(memory_space=pltpu.VMEM),
        scratch_shapes=[dma, dma, dma],
        compiler_params=pltpu.CompilerParams(collective_id=1, has_side_effects=True),
    )(attended)


def body(features, value_weight, output_weight, hit_list, sample_index, attention, validity):
    values = jnp.dot(features, value_weight, preferred_element_type=jnp.float32).astype(
        jnp.bfloat16
    )
    tiles = lax.axis_size("tile")
    cams = lax.axis_size("cam")
    place = lax.axis_index("cam")
    queries = sample_index.shape[0]
    width = values.shape[1]
    if cams == 2 and tiles in (4, 8, 12, 16) and width == 2 * LANES and features.shape[0] % 16 == 0:
        heads = H // 2
        vals = gather_values(values, tiles)
        index = lax.dynamic_slice_in_dim(sample_index, place * heads * K, heads * K, 2)
        attended = sample(
            hit_list, vals, index, attention, validity, heads, place * heads
        )
        attended = exchange(attended)
    else:
        share = queries // cams
        everything = lax.all_gather(values, ("tile", "cam"), axis=0, tiled=True)
        index, weights, valid = (
            lax.dynamic_slice_in_dim(a, place * share, share, 0)
            for a in (sample_index, attention, validity)
        )
        attended = sample(hit_list, everything, index, weights, valid, H, jnp.int32(0))
    return jnp.dot(attended, output_weight, preferred_element_type=jnp.float32).astype(jnp.bfloat16)


def solution(mesh):
    in_specs = (
        P(("tile", "cam"), None),
        P(),
        P(),
        P("tile", None),
        P("tile", None, None),
        P("tile", None),
        P("tile", None),
    )
    out_specs = P(("tile", "cam"), None)
    return jax.shard_map(body, mesh=mesh, in_specs=in_specs, out_specs=out_specs, check_vma=False)
```

```python
import functools

import jax
import jax.numpy as jnp
from jax import lax
from jax.experimental import pallas as pl
from jax.experimental.pallas import tpu as pltpu
from jax.sharding import PartitionSpec as P

H = 8
K = 8
HITS = 2
CAM_ROWS = 1024
LANES = 128
MESH = pl.DeviceIdType.MESH


def gather_kernel(depth, v_ref, G, recv, sx, sz, sy, sc):
    me = lax.axis_index("tile")
    x = lax.axis_index("cam")
    core = lax.rem(me, 2)
    y = lax.rem(me // 2, 2)
    z = me // 4
    rows, width = G.shape[0] // (depth * 8), G.shape[1]

    def half_of(index):
        return v_ref.at[:, pl.ds(pl.multiple_of(index * width, width), width)]

    def place(zz, yy, cc):
        return (zz * 2 + yy) * 2 + cc

    def block_of(zz, yy, cc, b):
        return place(zz, yy, cc) * 2 + b

    def span(blk):
        return pl.ds(pl.multiple_of(blk * rows, 16), rows)

    has_up = z < depth - 1
    has_down = z > 0
    x_peer = (me, 1 - x)
    y_peer = (place(z, 1 - y, core), x)
    c_peer = (place(z, y, 1 - core), x)
    has_up2 = z < depth - 2
    has_down2 = z > 1
    up_peer = (place(jnp.minimum(z + 1, depth - 1), y, core), x)
    down_peer = (place(jnp.maximum(z - 1, 0), y, core), x)
    up2_peer = (place(jnp.minimum(z + 2, depth - 1), y, core), x)
    down2_peer = (place(jnp.maximum(z - 2, 0), y, core), x)
    line = (
        (has_up2, up2_peer),
        (has_down2, down2_peer),
        (has_up, up_peer),
        (has_down, down_peer),
    )

    barrier = pltpu.get_barrier_semaphore()
    for peer in (x_peer, y_peer, c_peer):
        pl.semaphore_signal(barrier, inc=1, device_id=peer, device_id_type=MESH)

    peers = 3
    for exists, peer in line:
        peers = peers + exists.astype(jnp.int32)

        @pl.when(exists)
        def _(peer=peer):
            pl.semaphore_signal(barrier, inc=1, device_id=peer, device_id_type=MESH)

    pl.semaphore_wait(barrier, peers)

    def copy(src, blk, send, peer):
        return pltpu.make_async_remote_copy(
            src_ref=src,
            dst_ref=G.at[span(blk)],
            send_sem=send,
            recv_sem=recv.at[blk],
            device_id=peer,
            device_id_type=MESH,
        )

    def arrived(blk):
        copy(G.at[span(blk)], blk, sx.at[0], x_peer).wait_recv()

    own = block_of(z, y, core, x)
    copy(half_of(1 - x), own, sx.at[0], x_peer).start()

    def send_line(which, src, blk, slot):
        exists, peer = line[which]

        @pl.when(exists)
        def _():
            copy(src, blk, sz.at[slot], peer).start()

    def line_step(distance):
        for sign in (1, -1) if distance else (0,):
            zz = z - sign * distance
            live = (zz >= 0) & (zz < depth)
            for b in (0, 1):
                half = x if b == 0 else 1 - x

                def go(zz=zz, half=half, b=b, sign=sign):
                    blk = block_of(zz, y, core, half)
                    if distance == 0 and b == 0:
                        src = half_of(x)
                    else:
                        arrived(blk)
                        src = G.at[span(blk)]
                    slot = zz * 2 + half
                    if distance == 0:
                        for which in range(4):
                            send_line(which, src, blk, which * 2 + b)
                    elif distance == 2:
                        which = 2 if sign > 0 else 3
                        send_line(which, src, blk, 4 + which * 2 + b)
                    copy(src, blk, sy.at[slot], y_peer).start()
                    copy(src, blk, sc.at[slot], c_peer).start()

                if distance:
                    pl.when(live)(go)
                else:
                    go()

    def across_step(distance):
        for sign in (1, -1) if distance else (0,):
            zz = z - sign * distance
            live = (zz >= 0) & (zz < depth)
            for b in (0, 1):
                half = x if b == 0 else 1 - x

                def go(zz=zz, half=half):
                    blk = block_of(zz, 1 - y, core, half)
                    arrived(blk)
                    slot = depth * 2 + zz * 2 + half
                    copy(G.at[span(blk)], blk, sc.at[slot], c_peer).start()

                if distance:
                    pl.when(live)(go)
                else:
                    go()

    for distance in range(depth):
        line_step(distance)
        if distance:
            across_step(distance - 1)
    G[span(own), :] = v_ref[:, pl.ds(pl.multiple_of(x * width, width), width)]
    across_step(depth - 1)

    for zz in range(depth):
        for yy in (0, 1):
            for b in (0, 1):
                arrived(block_of(zz, yy, 1 - core, b))

    def sent(sem):
        copy(half_of(0), own, sem, x_peer).wait_send()

    sent(sx.at[0])
    for slot in range(depth * 2):
        sent(sy.at[slot])
    for b in (0, 1):
        for which in range(4):
            pl.when(line[which][0])(lambda i=which * 2 + b: sent(sz.at[i]))
        pl.when(has_up & has_down2)(lambda b=b: sent(sz.at[8 + b]))
        pl.when(has_down & has_up2)(lambda b=b: sent(sz.at[10 + b]))
    for slot in range(depth * 4):
        sent(sc.at[slot])


def gather_values(values, tiles):
    depth = tiles // 4
    rows, width = values.shape[0], values.shape[1] // 2
    blocks = tiles * 2
    dma = pltpu.SemaphoreType.DMA
    return pl.pallas_call(
        functools.partial(gather_kernel, depth),
        out_shape=jax.ShapeDtypeStruct((blocks * rows, width), jnp.bfloat16),
        in_specs=[pl.BlockSpec(memory_space=pltpu.VMEM)],
        out_specs=pl.BlockSpec(memory_space=pltpu.VMEM),
        scratch_shapes=[
            dma((blocks,)),
            dma((1,)),
            dma((12,)),
            dma((depth * 2,)),
            dma((depth * 4,)),
        ],
        compiler_params=pltpu.CompilerParams(collective_id=0, has_side_effects=True),
    )(values)


def lane_pick(source, index):
    return jnp.take_along_axis(source, index, axis=1, mode="promise_in_bounds")


def sample_kernel(
    heads, pair, hit_ref, head_ref, vals_ref, idx_ref, attn_ref, valid_ref, out_ref, table, attns, summed
):
    width = vals_ref.shape[1]
    head_width = width // heads
    queries = idx_ref.shape[1]
    groups = queries // LANES
    parts = CAM_ROWS // LANES
    for s in range(HITS):
        for j in range(parts):
            first = pl.multiple_of(hit_ref[0, s] * CAM_ROWS + j * LANES, LANES)
            block = vals_ref[pl.ds(first, LANES), :].astype(jnp.float32)
            table[s * parts + j] = block.T
    attns[...] = attn_ref[...].astype(jnp.float32)

    def one(step, _):
        g = step * pair // heads
        lanes = pl.ds(pl.multiple_of(g * LANES, LANES), LANES)
        valid = valid_ref[:, lanes]
        count = jnp.maximum(jnp.sum(valid, axis=0, keepdims=True), 1)
        factor = valid.astype(jnp.float32) * (1.0 / count.astype(jnp.float32))
        for e in range(pair):
            h = lax.rem(step * pair, heads) + e
            attn = attns[pl.ds(pl.multiple_of((head_ref[0] + h) * K, K), K), lanes]
            acc = [jnp.zeros((8, LANES), jnp.float32)] * (head_width // 8)
            for s in range(HITS):
                index = idx_ref[pl.ds(pl.multiple_of(s * heads * K + h * K, K), K), lanes]
                low = index & (LANES - 1)
                high = index // LANES
                weight = attn * factor[s : s + 1]
                for k in range(K):
                    lo = jnp.broadcast_to(low[k : k + 1], (8, LANES))
                    hi = jnp.broadcast_to(high[k : k + 1], (8, LANES))
                    wt = jnp.broadcast_to(weight[k : k + 1], (8, LANES))
                    masks = [hi == j for j in range(parts)]
                    for d in range(head_width // 8):
                        cols = pl.ds(pl.multiple_of(h * head_width + d * 8, 8), 8)
                        picked = lane_pick(table[s * parts, cols, :], lo)
                        for j in range(1, parts):
                            got = lane_pick(table[s * parts + j, cols, :], lo)
                            picked = jnp.where(masks[j], got, picked)
                        acc[d] = acc[d] + wt * picked
            for d in range(head_width // 8):
                summed[pl.ds(pl.multiple_of(h * head_width + d * 8, 8), 8), :] = acc[d]

        @pl.when(lax.rem(step * pair, heads) == heads - pair)
        def _():
            rows = pl.ds(pl.multiple_of(g * LANES, LANES), LANES)
            out_ref[rows, :] = summed[...].T.astype(out_ref.dtype)

        return 0

    lax.fori_loop(0, groups * heads // pair, one, 0)


def sample(hit_list, vals, index, attention, validity, heads, first_head):
    queries = index.shape[0]
    width = vals.shape[1]
    padded = -(-queries // LANES) * LANES
    index = index.reshape(queries, HITS * heads * K).T
    extra = padded - queries
    index = jnp.pad(index, ((0, 0), (0, extra)))
    validity = jnp.pad(validity.T, ((0, 0), (0, extra)))
    attention = jnp.pad(attention.T, ((0, 0), (0, extra)))
    pair = 4 if heads % 4 == 0 else 1
    first_head = jnp.reshape(first_head, (1,)).astype(jnp.int32)
    out = pl.pallas_call(
        functools.partial(sample_kernel, heads, pair),
        out_shape=jax.ShapeDtypeStruct((padded, width), jnp.bfloat16),
        in_specs=[pl.BlockSpec(memory_space=pltpu.SMEM)] * 2
        + [pl.BlockSpec(memory_space=pltpu.VMEM)] * 4,
        out_specs=pl.BlockSpec(memory_space=pltpu.VMEM),
        scratch_shapes=[
            pltpu.VMEM((HITS * CAM_ROWS // LANES, width, LANES), jnp.float32),
            pltpu.VMEM(attention.shape, jnp.float32),
            pltpu.VMEM((width, LANES), jnp.float32),
        ],
    )(hit_list, first_head, vals, index, attention, validity)
    return out[:queries]


def exchange_kernel(a_ref, out_ref, local, send, recv):
    me = lax.axis_index("tile")
    x = lax.axis_index("cam")
    rows = out_ref.shape[0]
    width = a_ref.shape[1]
    peer = (me, 1 - x)
    barrier = pltpu.get_barrier_semaphore()
    pl.semaphore_signal(barrier, inc=1, device_id=peer, device_id_type=MESH)
    pl.semaphore_wait(barrier, 1)

    def share(index):
        return a_ref.at[pl.ds(pl.multiple_of(index * rows, rows), rows)]

    mine = out_ref.at[:, pl.ds(pl.multiple_of(x * width, width), width)]
    copy = pltpu.make_async_remote_copy(
        src_ref=share(1 - x),
        dst_ref=mine,
        send_sem=send,
        recv_sem=recv,
        device_id=peer,
        device_id_type=MESH,
    )
    copy.start()
    keep = pltpu.make_async_copy(share(x), mine, local)
    keep.start()
    keep.wait()
    copy.wait()


def exchange(attended):
    queries, width = attended.shape
    dma = pltpu.SemaphoreType.DMA
    return pl.pallas_call(
        exchange_kernel,
        out_shape=jax.ShapeDtypeStruct((queries // 2, width * 2), jnp.bfloat16),
        in_specs=[pl.BlockSpec(memory_space=pltpu.VMEM)],
        out_specs=pl.BlockSpec(memory_space=pltpu.VMEM),
        scratch_shapes=[dma, dma, dma],
        compiler_params=pltpu.CompilerParams(collective_id=1, has_side_effects=True),
    )(attended)


def body(features, value_weight, output_weight, hit_list, sample_index, attention, validity):
    values = jnp.dot(features, value_weight, preferred_element_type=jnp.float32).astype(
        jnp.bfloat16
    )
    tiles = lax.axis_size("tile")
    cams = lax.axis_size("cam")
    place = lax.axis_index("cam")
    queries = sample_index.shape[0]
    width = values.shape[1]
    if cams == 2 and tiles in (4, 8, 12, 16) and width == 2 * LANES and features.shape[0] % 16 == 0:
        heads = H // 2
        vals = gather_values(values, tiles)
        index = lax.dynamic_slice_in_dim(sample_index, place * heads * K, heads * K, 2)
        attended = sample(
            hit_list, vals, index, attention, validity, heads, place * heads
        )
        attended = exchange(attended)
    else:
        share = queries // cams
        everything = lax.all_gather(values, ("tile", "cam"), axis=0, tiled=True)
        index, weights, valid = (
            lax.dynamic_slice_in_dim(a, place * share, share, 0)
            for a in (sample_index, attention, validity)
        )
        attended = sample(hit_list, everything, index, weights, valid, H, jnp.int32(0))
    return jnp.dot(attended, output_weight, preferred_element_type=jnp.float32).astype(jnp.bfloat16)


def solution(mesh):
    in_specs = (
        P(("tile", "cam"), None),
        P(),
        P(),
        P("tile", None),
        P("tile", None, None),
        P("tile", None),
        P("tile", None),
    )
    out_specs = P(("tile", "cam"), None)
    return jax.shard_map(body, mesh=mesh, in_specs=in_specs, out_specs=out_specs, check_vma=False)
```
